32 devices in a mesh: pb: 4 (over x, core), dev: 8 (over z, y).
Axes of the slice: x: 2, y: 2, z: 4, core: 2. Of those that a mesh axis runs over, the one named last changes fastest.
Arguments:
- queries: bfloat16 [1024, 128], P(('dev', 'pb')), may hold values from -0.75 to 0.75
- documents: bfloat16 [8192, 128], P(('pb', 'dev')), may hold values from -0.75 to 0.75
- lengths: int32 [64], P(('pb', 'dev')), may hold values from 1 to 128
- normalizers: float32 [64, 1024], P('pb', 'dev'), may hold values from 4.5 to 7.5
- probs: float32 [32, 64], P('dev', 'pb'), may hold values from 0.01 to 0.2
- positives: int32 [32], P('dev'), may hold values from 0 to 63
Outputs:
- query_grad: float32 [1024, 128], P(('dev', 'pb'))
- doc_grad: float32 [8192, 128], P(('pb', 'dev'))
The draws below stay inside these ranges and needn't reach their ends.
Inputs may be any that keep to these rules, and one draw needn't show every extreme that they name: `lengths`: slots of a document at positions of its length or beyond are padding. `positives`: index of the query's paired document among all 64.
All inputs are finite; a program needn't handle non-finite values.
Results may differ from the reference program's by a relative error of at most 0.00082.
Values may be sent and summed in bfloat16 or wider, within the bound.
A program may use at most 64 MiB of HBM per device.

```python
import math
import jax
import jax.numpy as jnp
from jax import lax

E = 128
LQ = 32
LD = 128
QUERIES = 32
DOCS = 64
QTOKENS = 1024
DTOKENS = 8192
N_DEV = 8


def place_ends(array, own_key, least, top_value):
    dims = array.shape
    spot = [jax.random.randint(jax.random.fold_in(own_key, axis), (), 0, dims[axis]) for axis in range(len(dims))]
    array = array.at[tuple(spot)].set(least)
    longest = dims.index(max(dims))
    spot[longest] = (spot[longest] + 1) % dims[longest]
    return array.at[tuple(spot)].set(top_value)


def levels(stream_key, extent, pieces, least, largest):
    loudness = 1.0
    for position, blocks in pieces:
        draws = jax.random.uniform(jax.random.fold_in(jax.random.fold_in(stream_key, 6), position), (blocks,), jnp.float32, least / len(pieces), largest / len(pieces))
        loudness = loudness * jnp.repeat(jnp.exp(draws), extent[position] // blocks).reshape((-1,) + (1,) * (len(extent) - 1 - position))
    return loudness


def gaussian(stream_key, extent, spread, reach, shards=(), kind=jnp.bfloat16):
    array = jax.random.normal(stream_key, extent, jnp.float32) * spread
    if len(shards) > 0:
        array = levels(stream_key, extent, shards, -0.22, 0.18) * array
    return jnp.clip(array, min=-reach, max=reach).astype(kind)


def setup_inputs(seed: int = 0) -> dict:
    keys = jax.random.split(jax.random.key(seed), 7)
    queries = gaussian(keys[0], (QTOKENS, E), 0.125, 0.75, ((0, 32),))
    documents = gaussian(keys[1], (DTOKENS, E), 0.125, 0.75, ((0, 32),))
    lengths = place_ends(jax.random.randint(keys[2], (DOCS,), 1, LD + 1), jax.random.fold_in(keys[2], 1), 1, LD).astype(jnp.int32)
    normalizers = jnp.clip(4.5 + 3.0 * jax.random.uniform(keys[3], (DOCS, QTOKENS), jnp.float32) ** levels(keys[3], (DOCS, QTOKENS), ((0, 4), (1, 8)), -0.2, 0.2), 4.5, 7.5)
    probs = jnp.clip(jnp.exp(math.log(0.2) - 2.9957323 * jax.random.uniform(keys[4], (QUERIES, DOCS), jnp.float32) ** levels(keys[4], (QUERIES, DOCS), ((0, 8), (1, 4)), -0.2, 0.2)), 0.01, 0.2)
    positives = place_ends(jax.random.randint(keys[5], (QUERIES,), 0, DOCS), jax.random.fold_in(keys[5], 1), 0, DOCS - 1).astype(jnp.int32)
    return {"queries": queries, "documents": documents, "lengths": lengths, "normalizers": normalizers, "probs": probs, "positives": positives}


sharpness = 10.0


def interact(query_rows, z_rows, p_cols, positive_ids, doc_rows, doc_lengths, first_doc):
    query_total = query_rows.shape[0]
    query_count = p_cols.shape[0]
    query_length = query_total // query_count
    doc_count = doc_lengths.shape[0]
    doc_length = doc_rows.shape[0] // doc_count
    scores = lax.dot_general(query_rows, doc_rows, (((1,), (1,)), ((), ())), preferred_element_type=jnp.float32)
    scores = scores.reshape(query_count, query_length, doc_count, doc_length)
    doc_ids = first_doc + jnp.arange(doc_count, dtype=jnp.int32)
    signal = p_cols - (positive_ids[:, None] == doc_ids[None, :]).astype(jnp.float32)
    present = (jnp.arange(doc_length, dtype=jnp.int32)[None, :] < doc_lengths[:, None]).astype(jnp.float32)
    z_cols = jnp.transpose(z_rows.reshape(doc_count, query_count, query_length), (1, 2, 0))
    shifted = sharpness * scores - z_cols[:, :, :, None]
    shifted = jnp.minimum(shifted, 0.0)
    weight = jnp.exp(shifted) * present[None, None] * signal[:, None, :, None]
    weight = weight.reshape(query_total, doc_count * doc_length).astype(jnp.bfloat16)
    query_part = jnp.dot(weight, doc_rows, preferred_element_type=jnp.float32)
    doc_part = lax.dot_general(weight, query_rows, (((0,), (0,)), ((), ())), preferred_element_type=jnp.float32)
    return query_part, doc_part


def reference(queries, documents, lengths, normalizers, probs, positives):
    group_count = N_DEV
    query_count = QUERIES // group_count
    token_count = query_count * LQ

    def one_group(doc_total, inputs):
        query_rows, z_rows, p_rows, positive_ids = inputs
        query_part, doc_part = interact(query_rows, z_rows, p_rows, positive_ids, documents, lengths, jnp.int32(0))
        return doc_total + doc_part, query_part

    stacked = (queries.reshape(group_count, token_count, E),
               jnp.transpose(normalizers.reshape(DOCS, group_count, token_count), (1, 0, 2)),
               probs.reshape(group_count, query_count, DOCS),
               positives.reshape(group_count, query_count))
    doc_grad, query_parts = lax.scan(one_group, jnp.zeros((DTOKENS, E), jnp.float32), stacked)
    return query_parts.reshape(QTOKENS, E), doc_grad
```

```python
import functools

import jax
import jax.numpy as jnp
from jax import lax
from jax.experimental import pallas as pl
from jax.experimental.pallas import tpu as pltpu
from jax.sharding import PartitionSpec as P

sharpness = 10.0
MESH = pl.DeviceIdType.MESH
F32 = jnp.float32


def kernel(
    n_pb,
    n_dev,
    queries,
    documents,
    lengths,
    normalizers,
    probs,
    positives,
    query_out,
    doc_out,
    q_own,
    d_own,
    z_own,
    q_all,
    d_all,
    aux_send,
    aux_recv,
    aux_turn,
    aux_all,
    doc_part,
    pair_recv,
    pair_sum,
    chip_recv,
    q_part,
    q_recv,
    in_sem,
    q_ss,
    q_rs,
    a_ss,
    a_rs,
    d_ss,
    d_rs,
    t_ss,
    t_rs,
    e_ss,
    e_rs,
    c_ss,
    c_rs,
    r_ss,
    r_rs,
):
    my_pb = lax.axis_index("pb")
    my_dev = lax.axis_index("dev")
    own_docs = lengths.shape[0]
    slots = d_own.shape[0] // own_docs
    row_docs, block = z_own.shape
    tokens = q_own.shape[0]
    block_queries = probs.shape[0]
    query_length = block // block_queries
    n_chip = n_pb // 2
    my_chip, my_core = my_pb // 2, my_pb % 2
    partner = my_chip * 2 + (1 - my_core)

    def dev_mate(step):
        return lax.rem(my_dev + step, n_dev)

    def pb_mate(step):
        return lax.rem(my_pb + step, n_pb)

    def chip_mate(step):
        return lax.rem(my_chip + step, n_chip)

    def remote(src, dst, send, recv, pb=None, dev=None):
        return pltpu.make_async_remote_copy(
            src_ref=src,
            dst_ref=dst,
            send_sem=send,
            recv_sem=recv,
            device_id=(my_pb if pb is None else pb, my_dev if dev is None else dev),
            device_id_type=MESH,
        )

    barrier = pltpu.get_barrier_semaphore()
    for step in range(1, n_dev):
        pl.semaphore_signal(
            barrier, inc=1, device_id=(my_pb, dev_mate(step)), device_id_type=MESH
        )
    for step in range(1, n_pb):
        pl.semaphore_signal(
            barrier, inc=1, device_id=(pb_mate(step), my_dev), device_id_type=MESH
        )

    loads = [
        pltpu.make_async_copy(queries, q_own, in_sem.at[0]),
        pltpu.make_async_copy(documents, d_own, in_sem.at[1]),
        pltpu.make_async_copy(normalizers, z_own, in_sem.at[2]),
    ]
    for load in loads:
        load.start()
    for load in loads:
        load.wait()

    place0 = lax.broadcasted_iota(jnp.int32, (row_docs, row_docs), 0)
    place1 = lax.broadcasted_iota(jnp.int32, (row_docs, row_docs), 1)
    doc_ids = my_pb * row_docs + lax.broadcasted_iota(jnp.int32, (row_docs, 1), 0)
    query_of = lax.broadcasted_iota(jnp.int32, (1, block), 1) // query_length
    signal = jnp.zeros((row_docs, block), F32)
    for k in range(block_queries):
        column = jnp.sum(
            jnp.where(place0 == place1, probs[k : k + 1, :], 0.0), axis=1, keepdims=True
        )
        column = column - (doc_ids == positives[k]).astype(F32)
        signal = jnp.where(query_of == k, column, signal)
    for e in range(n_dev):
        span = slice(e * own_docs, (e + 1) * own_docs)
        aux_send[e, 0:own_docs, :] = z_own[span, :]
        aux_send[e, own_docs : 2 * own_docs, :] = signal[span, :]
    aux_recv[my_dev] = aux_send[my_dev]
    q_all[my_dev] = q_own[...]

    slot = lax.broadcasted_iota(jnp.int32, (slots, 1), 0)
    for k in range(own_docs):
        span = slice(k * slots, (k + 1) * slots)
        rows = d_own[span, :].astype(F32)
        d_all[my_pb, span, :] = jnp.where(slot < lengths[k], rows, 0.0).astype(jnp.bfloat16)

    pl.semaphore_wait(barrier, n_dev - 1 + n_pb - 1)

    aux_copies, q_copies, d_copies = [], [], []
    for step in range(1, n_dev):
        mate = dev_mate(step)
        copy = remote(
            aux_send.at[mate], aux_recv.at[my_dev], a_ss.at[step], a_rs.at[step], dev=mate
        )
        copy.start()
        aux_copies.append(copy)
    for step in range(1, n_dev):
        copy = remote(q_own, q_all.at[my_dev], q_ss.at[step], q_rs.at[step], dev=dev_mate(step))
        copy.start()
        q_copies.append(copy)
    for step in range(1, n_pb):
        copy = remote(
            d_all.at[my_pb], d_all.at[my_pb], d_ss.at[step], d_rs.at[step], pb=pb_mate(step)
        )
        copy.start()
        d_copies.append(copy)

    for copy in aux_copies:
        copy.wait_recv()
    for p in range(n_pb):
        for e in range(n_dev):
            aux_turn[p, :, e * tokens : (e + 1) * tokens] = aux_recv[
                e, :, p * tokens : (p + 1) * tokens
            ]
    aux_all[my_pb] = aux_turn[my_pb]
    turn_copies = []
    for step in range(1, n_pb):
        mate = pb_mate(step)
        copy = remote(
            aux_turn.at[mate], aux_all.at[my_pb], t_ss.at[step], t_rs.at[step], pb=mate
        )
        copy.start()
        turn_copies.append(copy)

    for copy in q_copies + d_copies + turn_copies:
        copy.wait_recv()

    q_rows = q_all[...].reshape(n_dev * tokens, q_own.shape[1])

    def interact(p, total):
        d_rows = d_all[p]
        scores = lax.dot_general(
            d_rows, q_rows, (((1,), (1,)), ((), ())), preferred_element_type=F32
        )
        aux = aux_all[p]
        parts = []
        for k in range(own_docs):
            shifted = sharpness * scores[k * slots : (k + 1) * slots, :] - aux[k : k + 1, :]
            weight = jnp.exp(jnp.minimum(shifted, 0.0)) * aux[own_docs + k : own_docs + k + 1, :]
            parts.append(weight.astype(jnp.bfloat16))
        weight = jnp.concatenate(parts, axis=0)
        doc_part[p] = jnp.dot(weight, q_rows, preferred_element_type=F32)
        return total + lax.dot_general(
            weight, d_rows, (((0,), (0,)), ((), ())), preferred_element_type=F32
        )

    total = jnp.zeros((n_dev * tokens, q_own.shape[1]), F32)
    pair_copies = []

    def send_pair(step):
        copy = remote(
            doc_part.at[chip_mate(step) * 2 + (1 - my_core)],
            pair_recv.at[step],
            e_ss.at[step],
            e_rs.at[step],
            pb=partner,
        )
        copy.start()
        pair_copies.append(copy)

    if n_chip <= 2:
        for step in range(1, n_chip):
            for core in range(2):
                total = interact(chip_mate(step) * 2 + core, total)
            send_pair(step)
        for core in range(2):
            total = interact(my_chip * 2 + core, total)
        send_pair(0)
    else:
        total = lax.fori_loop(0, n_pb, interact, total)
        for step in list(range(1, n_chip)) + [0]:
            send_pair(step)
    q_part[...] = total.reshape(q_part.shape)

    out_copies = []
    for step in range(1, n_dev):
        mate = dev_mate(step)
        copy = remote(q_part.at[mate], q_recv.at[my_dev], r_ss.at[step], r_rs.at[step], dev=mate)
        copy.start()
        out_copies.append(copy)
    q_recv[my_dev] = q_part[my_dev]

    chip_copies = []
    for step in range(1, n_chip):
        pair_copies[step - 1].wait_recv()
        pair_sum[step] = doc_part[chip_mate(step) * 2 + my_core] + pair_recv[step]
        copy = remote(
            pair_sum.at[step],
            chip_recv.at[step],
            c_ss.at[step],
            c_rs.at[step],
            pb=chip_mate(step) * 2 + my_core,
        )
        copy.start()
        chip_copies.append(copy)
    pair_copies[-1].wait_recv()
    doc_total = doc_part[my_pb] + pair_recv[0]
    for step in range(1, n_chip):
        chip_copies[step - 1].wait_recv()
        doc_total = doc_total + chip_recv[step]
    for k in range(own_docs):
        span = slice(k * slots, (k + 1) * slots)
        doc_out[span, :] = jnp.where(slot < lengths[k], doc_total[span, :], 0.0)

    for copy in out_copies:
        copy.wait_recv()
    query_total = q_recv[0]
    for e in range(1, n_dev):
        query_total = query_total + q_recv[e]
    query_out[...] = query_total

    for copy in (
        aux_copies + q_copies + d_copies + turn_copies + pair_copies + out_copies + chip_copies
    ):
        copy.wait_send()


def per_device(queries, documents, lengths, normalizers, probs, positives):
    n_pb, n_dev = lax.axis_size("pb"), lax.axis_size("dev")
    tokens, width = queries.shape
    rows = documents.shape[0]
    own_docs = lengths.shape[0]
    block = normalizers.shape[1]
    n_chip = n_pb // 2
    bf16 = jnp.bfloat16
    dma = pltpu.SemaphoreType.DMA
    hbm = pl.BlockSpec(memory_space=pl.ANY)
    vmem = pl.BlockSpec(memory_space=pltpu.VMEM)
    smem = pl.BlockSpec(memory_space=pltpu.SMEM)
    return pl.pallas_call(
        functools.partial(kernel, n_pb, n_dev),
        out_shape=(
            jax.ShapeDtypeStruct((tokens, width), F32),
            jax.ShapeDtypeStruct((rows, width), F32),
        ),
        in_specs=[hbm, hbm, smem, hbm, vmem, smem],
        out_specs=(vmem, vmem),
        scratch_shapes=[
            pltpu.VMEM((tokens, width), bf16),
            pltpu.VMEM((rows, width), bf16),
            pltpu.VMEM(normalizers.shape, F32),
            pltpu.VMEM((n_dev, tokens, width), bf16),
            pltpu.VMEM((n_pb, rows, width), bf16),
            pltpu.VMEM((n_dev, 2 * own_docs, block), F32),
            pltpu.VMEM((n_dev, 2 * own_docs, block), F32),
            pltpu.VMEM((n_pb, 2 * own_docs, n_dev * tokens), F32),
            pltpu.VMEM((n_pb, 2 * own_docs, n_dev * tokens), F32),
            pltpu.VMEM((n_pb, rows, width), F32),
            pltpu.VMEM((n_chip, rows, width), F32),
            pltpu.VMEM((n_chip, rows, width), F32),
            pltpu.VMEM((n_chip, rows, width), F32),
            pltpu.VMEM((n_dev, tokens, width), F32),
            pltpu.VMEM((n_dev, tokens, width), F32),
            dma((3,)),
        ]
        + [dma((n_dev,))] * 4
        + [dma((n_pb,))] * 4
        + [dma((n_chip,))] * 4
        + [dma((n_dev,))] * 2,
        compiler_params=pltpu.CompilerParams(collective_id=0, has_side_effects=True),
    )(queries, documents, lengths, normalizers, probs, positives)


def solution(mesh):
    in_specs = (
        P(("dev", "pb"), None),
        P(("pb", "dev"), None),
        P(("pb", "dev")),
        P("pb", "dev"),
        P("dev", "pb"),
        P("dev"),
    )
    out_specs = (P(("dev", "pb"), None), P(("pb", "dev"), None))
    return jax.shard_map(
        per_device, mesh=mesh, in_specs=in_specs, out_specs=out_specs, check_vma=False
    )
```

```python
import functools

import jax
import jax.numpy as jnp
from jax import lax
from jax.experimental import pallas as pl
from jax.experimental.pallas import tpu as pltpu
from jax.sharding import PartitionSpec as P

sharpness = 10.0
MESH = pl.DeviceIdType.MESH
F32 = jnp.float32


def kernel(
    n_pb,
    n_dev,
    queries,
    documents,
    lengths_in,
    normalizers,
    probs_in,
    positives_in,
    query_out,
    doc_out,
    lengths,
    probs,
    positives,
    scores,
    q_own,
    d_own,
    z_own,
    q_all,
    d_all,
    aux_send,
    aux_recv,
    aux_turn,
    aux_all,
    doc_part,
    pair_recv,
    pair_sum,
    chip_recv,
    q_part,
    q_recv,
    in_sem,
    q_ss,
    q_rs,
    a_ss,
    a_rs,
    d_ss,
    d_rs,
    t_ss,
    t_rs,
    e_ss,
    e_rs,
    c_ss,
    c_rs,
    r_ss,
    r_rs,
):
    my_pb = lax.axis_index("pb")
    my_dev = lax.axis_index("dev")
    own_docs = lengths.shape[0]
    slots = d_own.shape[0] // own_docs
    row_docs, block = z_own.shape
    tokens = q_own.shape[0]
    block_queries = probs.shape[0]
    query_length = block // block_queries
    n_chip = n_pb // 2
    my_chip, my_core = my_pb // 2, my_pb % 2
    partner = my_chip * 2 + (1 - my_core)

    def crossed(place, step, count):
        mate, bit = 0, 1
        while bit < count:
            mate = mate + bit * ((place // bit + step // bit) % 2)
            bit *= 2
        return mate

    def dev_mate(step):
        return crossed(my_dev, step, n_dev)

    def pb_mate(step):
        return crossed(my_pb, step, n_pb)

    def chip_mate(step):
        return crossed(my_chip, step, n_chip)

    def remote(src, dst, send, recv, pb=None, dev=None):
        return pltpu.make_async_remote_copy(
            src_ref=src,
            dst_ref=dst,
            send_sem=send,
            recv_sem=recv,
            device_id=(my_pb if pb is None else pb, my_dev if dev is None else dev),
            device_id_type=MESH,
        )

    barrier = pltpu.get_barrier_semaphore()
    far_first = list(range(n_dev - 1, 0, -1))
    for step in far_first:
        pl.semaphore_signal(
            barrier, inc=1, device_id=(my_pb, dev_mate(step)), device_id_type=MESH
        )
    for step in range(1, n_pb):
        pl.semaphore_signal(
            barrier, inc=1, device_id=(pb_mate(step), my_dev), device_id_type=MESH
        )

    loads = [
        pltpu.make_async_copy(queries, q_own, in_sem.at[0]),
        pltpu.make_async_copy(documents, d_own, in_sem.at[1]),
        pltpu.make_async_copy(normalizers, z_own, in_sem.at[2]),
        pltpu.make_async_copy(lengths_in, lengths, in_sem.at[3]),
        pltpu.make_async_copy(probs_in, probs, in_sem.at[4]),
        pltpu.make_async_copy(positives_in, positives, in_sem.at[5]),
    ]
    for load in loads:
        load.start()
    for load in loads:
        load.wait()

    place0 = lax.broadcasted_iota(jnp.int32, (row_docs, row_docs), 0)
    place1 = lax.broadcasted_iota(jnp.int32, (row_docs, row_docs), 1)
    doc_ids = my_pb * row_docs + lax.broadcasted_iota(jnp.int32, (row_docs, 1), 0)
    query_of = lax.broadcasted_iota(jnp.int32, (1, block), 1) // query_length
    signal = jnp.zeros((row_docs, block), F32)
    for k in range(block_queries):
        column = jnp.sum(
            jnp.where(place0 == place1, probs[k : k + 1, :], 0.0), axis=1, keepdims=True
        )
        column = column - (doc_ids == positives[k]).astype(F32)
        signal = jnp.where(query_of == k, column, signal)
    for e in range(n_dev):
        span = slice(e * own_docs, (e + 1) * own_docs)
        aux_send[e, 0:own_docs, :] = z_own[span, :]
        aux_send[e, own_docs : 2 * own_docs, :] = signal[span, :]
    aux_recv[my_dev] = aux_send[my_dev]
    q_all[my_dev] = q_own[...]

    slot = lax.broadcasted_iota(jnp.int32, (slots, 1), 0)
    for k in range(own_docs):
        span = slice(k * slots, (k + 1) * slots)
        rows = d_own[span, :].astype(F32)
        d_all[my_pb, span, :] = jnp.where(slot < lengths[k], rows, 0.0).astype(jnp.bfloat16)

    pl.semaphore_wait(barrier, n_dev - 1 + n_pb - 1)

    aux_copies, q_copies, d_copies = [], [], []
    for step in far_first:
        mate = dev_mate(step)
        copy = remote(
            aux_send.at[mate], aux_recv.at[my_dev], a_ss.at[step], a_rs.at[step], dev=mate
        )
        copy.start()
        aux_copies.append(copy)
    for step in far_first:
        copy = remote(q_own, q_all.at[my_dev], q_ss.at[step], q_rs.at[step], dev=dev_mate(step))
        copy.start()
        q_copies.append(copy)
    for step in range(1, n_pb):
        copy = remote(
            d_all.at[my_pb], d_all.at[my_pb], d_ss.at[step], d_rs.at[step], pb=pb_mate(step)
        )
        copy.start()
        d_copies.append(copy)

    for copy in aux_copies:
        copy.wait_recv()
    for p in range(n_pb):
        for e in range(n_dev):
            aux_turn[p, :, e * tokens : (e + 1) * tokens] = aux_recv[
                e, :, p * tokens : (p + 1) * tokens
            ]
    aux_all[my_pb] = aux_turn[my_pb]
    turn_copies = []
    for step in range(1, n_pb):
        mate = pb_mate(step)
        copy = remote(
            aux_turn.at[mate], aux_all.at[my_pb], t_ss.at[step], t_rs.at[step], pb=mate
        )
        copy.start()
        turn_copies.append(copy)

    for copy in q_copies + d_copies:
        copy.wait_recv()

    q_rows = q_all[...].reshape(n_dev * tokens, q_own.shape[1])

    def score(p):
        scores[p] = lax.dot_general(
            d_all[p], q_rows, (((1,), (1,)), ((), ())), preferred_element_type=F32
        )

    def interact(p, total):
        d_rows = d_all[p]
        aux = aux_all[p]
        parts = []
        for k in range(own_docs):
            shifted = sharpness * scores[p, k * slots : (k + 1) * slots, :] - aux[k : k + 1, :]
            weight = jnp.exp(jnp.minimum(shifted, 0.0)) * aux[own_docs + k : own_docs + k + 1, :]
            parts.append(weight.astype(jnp.bfloat16))
        weight = jnp.concatenate(parts, axis=0)
        doc_part[p] = jnp.dot(weight, q_rows, preferred_element_type=F32)
        return total + lax.dot_general(
            weight, d_rows, (((0,), (0,)), ((), ())), preferred_element_type=F32
        )

    total = jnp.zeros((n_dev * tokens, q_own.shape[1]), F32)
    pair_copies = []

    def send_pair(step):
        copy = remote(
            doc_part.at[chip_mate(step) * 2 + (1 - my_core)],
            pair_recv.at[step],
            e_ss.at[step],
            e_rs.at[step],
            pb=partner,
        )
        copy.start()
        pair_copies.append(copy)

    if n_chip <= 2:
        for step in range(0, n_pb):
            score(pb_mate(step))
        for copy in turn_copies:
            copy.wait_recv()
        total = interact(my_pb, total)
        for step in range(1, n_chip):
            for core in range(2):
                total = interact(chip_mate(step) * 2 + core, total)
            send_pair(step)
        total = interact(partner, total)
        send_pair(0)
    else:
        for copy in turn_copies:
            copy.wait_recv()
        lax.fori_loop(0, n_pb, lambda p, c: (score(p), c)[1], 0)
        total = lax.fori_loop(0, n_pb, interact, total)
        for step in list(range(1, n_chip)) + [0]:
            send_pair(step)
    q_part[...] = total.reshape(q_part.shape)

    out_copies = []
    for step in far_first:
        mate = dev_mate(step)
        copy = remote(q_part.at[mate], q_recv.at[my_dev], r_ss.at[step], r_rs.at[step], dev=mate)
        copy.start()
        out_copies.append(copy)
    q_recv[my_dev] = q_part[my_dev]

    chip_copies = []
    for step in range(1, n_chip):
        pair_copies[step - 1].wait_recv()
        pair_sum[step] = doc_part[chip_mate(step) * 2 + my_core] + pair_recv[step]
        copy = remote(
            pair_sum.at[step],
            chip_recv.at[step],
            c_ss.at[step],
            c_rs.at[step],
            pb=chip_mate(step) * 2 + my_core,
        )
        copy.start()
        chip_copies.append(copy)
    pair_copies[-1].wait_recv()
    doc_total = doc_part[my_pb] + pair_recv[0]
    for step in range(1, n_chip):
        chip_copies[step - 1].wait_recv()
        doc_total = doc_total + chip_recv[step]
    for k in range(own_docs):
        span = slice(k * slots, (k + 1) * slots)
        doc_out[span, :] = jnp.where(slot < lengths[k], doc_total[span, :], 0.0)

    for copy in out_copies:
        copy.wait_recv()
    query_total = q_recv[0]
    for e in range(1, n_dev):
        query_total = query_total + q_recv[e]
    query_out[...] = query_total

    for copy in (
        aux_copies + q_copies + d_copies + turn_copies + pair_copies + out_copies + chip_copies
    ):
        copy.wait_send()


def write_out(query_grad, doc_grad, query_out, doc_out, sem):
    copies = [
        pltpu.make_async_copy(query_grad, query_out, sem.at[0]),
        pltpu.make_async_copy(doc_grad, doc_out, sem.at[1]),
    ]
    for copy in copies:
        copy.start()
    for copy in copies:
        copy.wait()


def per_device(queries, documents, lengths, normalizers, probs, positives):
    n_pb, n_dev = lax.axis_size("pb"), lax.axis_size("dev")
    tokens, width = queries.shape
    rows = documents.shape[0]
    own_docs = lengths.shape[0]
    block = normalizers.shape[1]
    n_chip = n_pb // 2
    bf16 = jnp.bfloat16
    dma = pltpu.SemaphoreType.DMA
    hbm = pl.BlockSpec(memory_space=pl.ANY)
    vmem = pl.BlockSpec(memory_space=pltpu.VMEM)
    grads = pl.pallas_call(
        functools.partial(kernel, n_pb, n_dev),
        out_shape=(
            pltpu.VMEM((tokens, width), F32),
            pltpu.VMEM((rows, width), F32),
        ),
        in_specs=[hbm] * 6,
        out_specs=(vmem, vmem),
        scratch_shapes=[
            pltpu.SMEM(lengths.shape, jnp.int32),
            pltpu.VMEM(probs.shape, F32),
            pltpu.SMEM(positives.shape, jnp.int32),
            pltpu.VMEM((n_pb, rows, n_dev * tokens), F32),
            pltpu.VMEM((tokens, width), bf16),
            pltpu.VMEM((rows, width), bf16),
            pltpu.VMEM(normalizers.shape, F32),
            pltpu.VMEM((n_dev, tokens, width), bf16),
            pltpu.VMEM((n_pb, rows, width), bf16),
            pltpu.VMEM((n_dev, 2 * own_docs, block), F32),
            pltpu.VMEM((n_dev, 2 * own_docs, block), F32),
            pltpu.VMEM((n_pb, 2 * own_docs, n_dev * tokens), F32),
            pltpu.VMEM((n_pb, 2 * own_docs, n_dev * tokens), F32),
            pltpu.VMEM((n_pb, rows, width), F32),
            pltpu.VMEM((n_chip, rows, width), F32),
            pltpu.VMEM((n_chip, rows, width), F32),
            pltpu.VMEM((n_chip, rows, width), F32),
            pltpu.VMEM((n_dev, tokens, width), F32),
            pltpu.VMEM((n_dev, tokens, width), F32),
            dma((6,)),
        ]
        + [dma((n_dev,))] * 4
        + [dma((n_pb,))] * 4
        + [dma((n_chip,))] * 4
        + [dma((n_dev,))] * 2,
        compiler_params=pltpu.CompilerParams(collective_id=0, has_side_effects=True),
    )(queries, documents, lengths, normalizers, probs, positives)
    return pl.pallas_call(
        write_out,
        out_shape=(
            jax.ShapeDtypeStruct((tokens, width), F32),
            jax.ShapeDtypeStruct((rows, width), F32),
        ),
        in_specs=[vmem, vmem],
        out_specs=(hbm, hbm),
        scratch_shapes=[dma((2,))],
    )(*grads)


def solution(mesh):
    in_specs = (
        P(("dev", "pb"), None),
        P(("pb", "dev"), None),
        P(("pb", "dev")),
        P("pb", "dev"),
        P("dev", "pb"),
        P("dev"),
    )
    out_specs = (P(("dev", "pb"), None), P(("pb", "dev"), None))
    return jax.shard_map(
        per_device, mesh=mesh, in_specs=in_specs, out_specs=out_specs, check_vma=False
    )
```

```python
import functools

import jax
import jax.numpy as jnp
from jax import lax
from jax.experimental import pallas as pl
from jax.experimental.pallas import tpu as pltpu
from jax.sharding import PartitionSpec as P

sharpness = 10.0
MESH = pl.DeviceIdType.MESH
F32 = jnp.float32


def kernel(
    n_pb,
    n_dev,
    queries,
    documents,
    lengths_in,
    normalizers,
    probs_in,
    positives_in,
    query_out,
    doc_out,
    lengths,
    probs,
    positives,
    scores,
    q_own,
    d_own,
    z_own,
    q_all,
    d_all,
    aux_send,
    aux_recv,
    aux_turn,
    aux_all,
    doc_part,
    pair_recv,
    pair_sum,
    chip_recv,
    q_part,
    q_recv,
    in_sem,
    q_ss,
    q_rs,
    a_ss,
    a_rs,
    d_ss,
    d_rs,
    t_ss,
    t_rs,
    e_ss,
    e_rs,
    c_ss,
    c_rs,
    r_ss,
    r_rs,
):
    my_pb = lax.axis_index("pb")
    my_dev = lax.axis_index("dev")
    own_docs = lengths.shape[0]
    slots = d_own.shape[0] // own_docs
    row_docs, block = z_own.shape
    tokens = q_own.shape[0]
    block_queries = probs.shape[0]
    query_length = block // block_queries
    n_chip = n_pb // 2
    my_chip, my_core = my_pb // 2, my_pb % 2
    partner = my_chip * 2 + (1 - my_core)

    def crossed(place, step, count):
        mate, bit = 0, 1
        while bit < count:
            mate = mate + bit * ((place // bit + step // bit) % 2)
            bit *= 2
        return mate

    def dev_mate(step):
        return crossed(my_dev, step, n_dev)

    def pb_mate(step):
        return crossed(my_pb, step, n_pb)

    def chip_mate(step):
        return crossed(my_chip, step, n_chip)

    def remote(src, dst, send, recv, pb=None, dev=None):
        return pltpu.make_async_remote_copy(
            src_ref=src,
            dst_ref=dst,
            send_sem=send,
            recv_sem=recv,
            device_id=(my_pb if pb is None else pb, my_dev if dev is None else dev),
            device_id_type=MESH,
        )

    barrier = pltpu.get_barrier_semaphore()
    far_first = list(range(n_dev - 1, 0, -1))
    for step in far_first:
        pl.semaphore_signal(
            barrier, inc=1, device_id=(my_pb, dev_mate(step)), device_id_type=MESH
        )
    for step in range(1, n_pb):
        pl.semaphore_signal(
            barrier, inc=1, device_id=(pb_mate(step), my_dev), device_id_type=MESH
        )

    loads = [
        pltpu.make_async_copy(queries, q_own, in_sem.at[0]),
        pltpu.make_async_copy(documents, d_own, in_sem.at[1]),
        pltpu.make_async_copy(normalizers, z_own, in_sem.at[2]),
        pltpu.make_async_copy(lengths_in, lengths, in_sem.at[3]),
        pltpu.make_async_copy(probs_in, probs, in_sem.at[4]),
        pltpu.make_async_copy(positives_in, positives, in_sem.at[5]),
    ]
    for load in loads:
        load.start()
    for load in loads:
        load.wait()

    place0 = lax.broadcasted_iota(jnp.int32, (row_docs, row_docs), 0)
    place1 = lax.broadcasted_iota(jnp.int32, (row_docs, row_docs), 1)
    doc_ids = my_pb * row_docs + lax.broadcasted_iota(jnp.int32, (row_docs, 1), 0)
    query_of = lax.broadcasted_iota(jnp.int32, (1, block), 1) // query_length
    signal = jnp.zeros((row_docs, block), F32)
    for k in range(block_queries):
        column = jnp.sum(
            jnp.where(place0 == place1, probs[k : k + 1, :], 0.0), axis=1, keepdims=True
        )
        column = column - (doc_ids == positives[k]).astype(F32)
        signal = jnp.where(query_of == k, column, signal)
    for e in range(n_dev):
        span = slice(e * own_docs, (e + 1) * own_docs)
        aux_send[e, 0:own_docs, :] = z_own[span, :]
        aux_send[e, own_docs : 2 * own_docs, :] = signal[span, :]
    aux_recv[my_dev] = aux_send[my_dev]
    q_all[my_dev] = q_own[...]

    slot = lax.broadcasted_iota(jnp.int32, (slots, 1), 0)
    for k in range(own_docs):
        span = slice(k * slots, (k + 1) * slots)
        rows = d_own[span, :].astype(F32)
        d_all[my_pb, span, :] = jnp.where(slot < lengths[k], rows, 0.0).astype(jnp.bfloat16)

    pl.semaphore_wait(barrier, n_dev - 1 + n_pb - 1)

    aux_copies, q_copies, d_copies = [], [], []
    for step in far_first:
        mate = dev_mate(step)
        copy = remote(
            aux_send.at[mate], aux_recv.at[my_dev], a_ss.at[step], a_rs.at[step], dev=mate
        )
        copy.start()
        aux_copies.append(copy)
    for step in far_first:
        copy = remote(q_own, q_all.at[my_dev], q_ss.at[step], q_rs.at[step], dev=dev_mate(step))
        copy.start()
        q_copies.append(copy)
    for step in range(1, n_pb):
        copy = remote(
            d_all.at[my_pb], d_all.at[my_pb], d_ss.at[step], d_rs.at[step], pb=pb_mate(step)
        )
        copy.start()
        d_copies.append(copy)

    for copy in aux_copies:
        copy.wait_recv()
    for p in range(n_pb):
        for e in range(n_dev):
            aux_turn[p, :, e * tokens : (e + 1) * tokens] = aux_recv[
                e, :, p * tokens : (p + 1) * tokens
            ]
    aux_all[my_pb] = aux_turn[my_pb]
    turn_copies = []
    for step in range(1, n_pb):
        mate = pb_mate(step)
        copy = remote(
            aux_turn.at[mate], aux_all.at[my_pb], t_ss.at[step], t_rs.at[step], pb=mate
        )
        copy.start()
        turn_copies.append(copy)

    for copy in q_copies + d_copies:
        copy.wait_recv()

    q_rows = q_all[...].reshape(n_dev * tokens, q_own.shape[1])

    def score(p):
        scores[p] = lax.dot_general(
            d_all[p], q_rows, (((1,), (1,)), ((), ())), preferred_element_type=F32
        )

    def interact(p, total):
        d_rows = d_all[p]
        aux = aux_all[p]
        parts = []
        for k in range(own_docs):
            shifted = sharpness * scores[p, k * slots : (k + 1) * slots, :] - aux[k : k + 1, :]
            weight = jnp.exp(jnp.minimum(shifted, 0.0)) * aux[own_docs + k : own_docs + k + 1, :]
            parts.append(weight.astype(jnp.bfloat16))
        weight = jnp.concatenate(parts, axis=0)
        doc_part[p] = jnp.dot(weight, q_rows, preferred_element_type=F32)
        return total + lax.dot_general(
            weight, d_rows, (((0,), (0,)), ((), ())), preferred_element_type=F32
        )

    total = jnp.zeros((n_dev * tokens, q_own.shape[1]), F32)
    pair_copies = []

    def send_pair(step):
        copy = remote(
            doc_part.at[chip_mate(step) * 2 + (1 - my_core)],
            pair_recv.at[step],
            e_ss.at[step],
            e_rs.at[step],
            pb=partner,
        )
        copy.start()
        pair_copies.append(copy)

    if n_chip <= 2:
        for step in range(0, n_pb):
            score(pb_mate(step))
        for copy in turn_copies:
            copy.wait_recv()
        total = interact(my_pb, total)
        for step in range(1, n_chip):
            for core in range(2):
                total = interact(chip_mate(step) * 2 + core, total)
            send_pair(step)
        total = interact(partner, total)
        send_pair(0)
    else:
        for copy in turn_copies:
            copy.wait_recv()
        lax.fori_loop(0, n_pb, lambda p, c: (score(p), c)[1], 0)
        total = lax.fori_loop(0, n_pb, interact, total)
        for step in list(range(1, n_chip)) + [0]:
            send_pair(step)
    q_part[...] = total.reshape(q_part.shape)

    out_copies = []
    for step in far_first:
        mate = dev_mate(step)
        copy = remote(q_part.at[mate], q_recv.at[my_dev], r_ss.at[step], r_rs.at[step], dev=mate)
        copy.start()
        out_copies.append(copy)
    q_recv[my_dev] = q_part[my_dev]

    chip_copies = []
    for step in range(1, n_chip):
        pair_copies[step - 1].wait_recv()
        pair_sum[step] = doc_part[chip_mate(step) * 2 + my_core] + pair_recv[step]
        copy = remote(
            pair_sum.at[step],
            chip_recv.at[step],
            c_ss.at[step],
            c_rs.at[step],
            pb=chip_mate(step) * 2 + my_core,
        )
        copy.start()
        chip_copies.append(copy)
    pair_copies[-1].wait_recv()
    doc_total = doc_part[my_pb] + pair_recv[0]
    for step in range(1, n_chip):
        chip_copies[step - 1].wait_recv()
        doc_total = doc_total + chip_recv[step]
    for k in range(own_docs):
        span = slice(k * slots, (k + 1) * slots)
        doc_out[span, :] = jnp.where(slot < lengths[k], doc_total[span, :], 0.0)

    for copy in out_copies:
        copy.wait_recv()
    query_total = q_recv[0]
    for e in range(1, n_dev):
        query_total = query_total + q_recv[e]
    query_out[...] = query_total

    for copy in (
        aux_copies + q_copies + d_copies + turn_copies + pair_copies + out_copies + chip_copies
    ):
        copy.wait_send()


def per_device(queries, documents, lengths, normalizers, probs, positives):
    n_pb, n_dev = lax.axis_size("pb"), lax.axis_size("dev")
    tokens, width = queries.shape
    rows = documents.shape[0]
    own_docs = lengths.shape[0]
    block = normalizers.shape[1]
    n_chip = n_pb // 2
    bf16 = jnp.bfloat16
    dma = pltpu.SemaphoreType.DMA
    hbm = pl.BlockSpec(memory_space=pl.ANY)
    vmem = pl.BlockSpec(memory_space=pltpu.VMEM)
    return pl.pallas_call(
        functools.partial(kernel, n_pb, n_dev),
        out_shape=(
            pltpu.VMEM((tokens, width), F32),
            pltpu.VMEM((rows, width), F32),
        ),
        in_specs=[hbm] * 6,
        out_specs=(vmem, vmem),
        scratch_shapes=[
            pltpu.SMEM(lengths.shape, jnp.int32),
            pltpu.VMEM(probs.shape, F32),
            pltpu.SMEM(positives.shape, jnp.int32),
            pltpu.VMEM((n_pb, rows, n_dev * tokens), F32),
            pltpu.VMEM((tokens, width), bf16),
            pltpu.VMEM((rows, width), bf16),
            pltpu.VMEM(normalizers.shape, F32),
            pltpu.VMEM((n_dev, tokens, width), bf16),
            pltpu.VMEM((n_pb, rows, width), bf16),
            pltpu.VMEM((n_dev, 2 * own_docs, block), F32),
            pltpu.VMEM((n_dev, 2 * own_docs, block), F32),
            pltpu.VMEM((n_pb, 2 * own_docs, n_dev * tokens), F32),
            pltpu.VMEM((n_pb, 2 * own_docs, n_dev * tokens), F32),
            pltpu.VMEM((n_pb, rows, width), F32),
            pltpu.VMEM((n_chip, rows, width), F32),
            pltpu.VMEM((n_chip, rows, width), F32),
            pltpu.VMEM((n_chip, rows, width), F32),
            pltpu.VMEM((n_dev, tokens, width), F32),
            pltpu.VMEM((n_dev, tokens, width), F32),
            dma((6,)),
        ]
        + [dma((n_dev,))] * 4
        + [dma((n_pb,))] * 4
        + [dma((n_chip,))] * 4
        + [dma((n_dev,))] * 2,
        compiler_params=pltpu.CompilerParams(collective_id=0, has_side_effects=True),
    )(queries, documents, lengths, normalizers, probs, positives)


def solution(mesh):
    in_specs = (
        P(("dev", "pb"), None),
        P(("pb", "dev"), None),
        P(("pb", "dev")),
        P("pb", "dev"),
        P("dev", "pb"),
        P("dev"),
    )
    out_specs = (P(("dev", "pb"), None), P(("pb", "dev"), None))
    return jax.shard_map(
        per_device, mesh=mesh, in_specs=in_specs, out_specs=out_specs, check_vma=False
    )
```

```python
import functools

import jax
import jax.numpy as jnp
from jax import lax
from jax.experimental import pallas as pl
from jax.experimental.pallas import tpu as pltpu
from jax.sharding import PartitionSpec as P

sharpness = 10.0
MESH = pl.DeviceIdType.MESH
F32 = jnp.float32


LEVELS = 32000.0


def encode(part):
    peak = jnp.maximum(jnp.max(jnp.abs(part), axis=1, keepdims=True), 1e-30)
    return jnp.round(part * (LEVELS / peak)).astype(jnp.int32).astype(jnp.int16), peak


def decode(code, peak):
    return code.astype(jnp.int32).astype(F32) * (peak * (1.0 / LEVELS))


def kernel(
    n_pb,
    n_dev,
    queries,
    documents,
    lengths_in,
    normalizers,
    probs_in,
    positives_in,
    query_out,
    doc_out,
    lengths,
    probs,
    positives,
    scores,
    q_own,
    d_own,
    z_own,
    q_all,
    d_all,
    aux_send,
    aux_recv,
    aux_turn,
    aux_all,
    doc_part,
    pair_recv,
    pair_code,
    pair_peak,
    chip_code,
    chip_peak,
    q_part,
    q_code,
    q_peak,
    q_recv,
    q_recv_peak,
    in_sem,
    q_ss,
    q_rs,
    a_ss,
    a_rs,
    d_ss,
    d_rs,
    t_ss,
    t_rs,
    e_ss,
    e_rs,
    c_ss,
    c_rs,
    r_ss,
    r_rs,
    rp_ss,
    rp_rs,
    cp_ss,
    cp_rs,
):
    my_pb = lax.axis_index("pb")
    my_dev = lax.axis_index("dev")
    own_docs = lengths.shape[0]
    slots = d_own.shape[0] // own_docs
    row_docs, block = z_own.shape
    tokens = q_own.shape[0]
    block_queries = probs.shape[0]
    query_length = block // block_queries
    n_chip = n_pb // 2
    my_chip, my_core = my_pb // 2, my_pb % 2
    partner = my_chip * 2 + (1 - my_core)

    def crossed(place, step, count):
        mate, bit = 0, 1
        while bit < count:
            mate = mate + bit * ((place // bit + step // bit) % 2)
            bit *= 2
        return mate

    def dev_mate(step):
        return crossed(my_dev, step, n_dev)

    def pb_mate(step):
        return crossed(my_pb, step, n_pb)

    def chip_mate(step):
        return crossed(my_chip, step, n_chip)

    def remote(src, dst, send, recv, pb=None, dev=None):
        return pltpu.make_async_remote_copy(
            src_ref=src,
            dst_ref=dst,
            send_sem=send,
            recv_sem=recv,
            device_id=(my_pb if pb is None else pb, my_dev if dev is None else dev),
            device_id_type=MESH,
        )

    barrier = pltpu.get_barrier_semaphore()
    far_first = list(range(n_dev - 1, 0, -1))
    for step in far_first:
        pl.semaphore_signal(
            barrier, inc=1, device_id=(my_pb, dev_mate(step)), device_id_type=MESH
        )
    for step in range(1, n_pb):
        pl.semaphore_signal(
            barrier, inc=1, device_id=(pb_mate(step), my_dev), device_id_type=MESH
        )

    loads = [
        pltpu.make_async_copy(queries, q_own, in_sem.at[0]),
        pltpu.make_async_copy(documents, d_own, in_sem.at[1]),
        pltpu.make_async_copy(normalizers, z_own, in_sem.at[2]),
        pltpu.make_async_copy(lengths_in, lengths, in_sem.at[3]),
        pltpu.make_async_copy(probs_in, probs, in_sem.at[4]),
        pltpu.make_async_copy(positives_in, positives, in_sem.at[5]),
    ]
    for load in loads:
        load.start()
    for load in loads:
        load.wait()

    place0 = lax.broadcasted_iota(jnp.int32, (row_docs, row_docs), 0)
    place1 = lax.broadcasted_iota(jnp.int32, (row_docs, row_docs), 1)
    doc_ids = my_pb * row_docs + lax.broadcasted_iota(jnp.int32, (row_docs, 1), 0)
    query_of = lax.broadcasted_iota(jnp.int32, (1, block), 1) // query_length
    signal = jnp.zeros((row_docs, block), F32)
    for k in range(block_queries):
        column = jnp.sum(
            jnp.where(place0 == place1, probs[k : k + 1, :], 0.0), axis=1, keepdims=True
        )
        column = column - (doc_ids == positives[k]).astype(F32)
        signal = jnp.where(query_of == k, column, signal)
    for e in range(n_dev):
        span = slice(e * own_docs, (e + 1) * own_docs)
        aux_send[e, 0:own_docs, :] = z_own[span, :]
        aux_send[e, own_docs : 2 * own_docs, :] = signal[span, :]
    aux_recv[my_dev] = aux_send[my_dev]
    q_all[my_dev] = q_own[...]

    slot = lax.broadcasted_iota(jnp.int32, (slots, 1), 0)
    for k in range(own_docs):
        span = slice(k * slots, (k + 1) * slots)
        rows = d_own[span, :].astype(F32)
        d_all[my_pb, span, :] = jnp.where(slot < lengths[k], rows, 0.0).astype(jnp.bfloat16)

    pl.semaphore_wait(barrier, n_dev - 1 + n_pb - 1)

    aux_copies, q_copies, d_copies = [], [], []
    for step in far_first:
        mate = dev_mate(step)
        copy = remote(
            aux_send.at[mate], aux_recv.at[my_dev], a_ss.at[step], a_rs.at[step], dev=mate
        )
        copy.start()
        aux_copies.append(copy)
    for step in far_first:
        copy = remote(q_own, q_all.at[my_dev], q_ss.at[step], q_rs.at[step], dev=dev_mate(step))
        copy.start()
        q_copies.append(copy)
    for step in range(1, n_pb):
        copy = remote(
            d_all.at[my_pb], d_all.at[my_pb], d_ss.at[step], d_rs.at[step], pb=pb_mate(step)
        )
        copy.start()
        d_copies.append(copy)

    for copy in aux_copies:
        copy.wait_recv()
    for p in range(n_pb):
        for e in range(n_dev):
            aux_turn[p, :, e * tokens : (e + 1) * tokens] = aux_recv[
                e, :, p * tokens : (p + 1) * tokens
            ]
    aux_all[my_pb] = aux_turn[my_pb]
    turn_copies = []
    for step in range(1, n_pb):
        mate = pb_mate(step)
        copy = remote(
            aux_turn.at[mate], aux_all.at[my_pb], t_ss.at[step], t_rs.at[step], pb=mate
        )
        copy.start()
        turn_copies.append(copy)

    for copy in q_copies + d_copies:
        copy.wait_recv()

    q_rows = q_all[...].reshape(n_dev * tokens, q_own.shape[1])

    def score(p):
        scores[p] = lax.dot_general(
            d_all[p], q_rows, (((1,), (1,)), ((), ())), preferred_element_type=F32
        )

    def interact(p, total):
        d_rows = d_all[p]
        aux = aux_all[p]
        parts = []
        for k in range(own_docs):
            shifted = sharpness * scores[p, k * slots : (k + 1) * slots, :] - aux[k : k + 1, :]
            weight = jnp.exp(jnp.minimum(shifted, 0.0)) * aux[own_docs + k : own_docs + k + 1, :]
            parts.append(weight.astype(jnp.bfloat16))
        weight = jnp.concatenate(parts, axis=0)
        doc_part[p] = jnp.dot(weight, q_rows, preferred_element_type=F32)
        return total + lax.dot_general(
            weight, d_rows, (((0,), (0,)), ((), ())), preferred_element_type=F32
        )

    total = jnp.zeros((n_dev * tokens, q_own.shape[1]), F32)
    pair_copies = []

    def send_pair(step):
        copy = remote(
            doc_part.at[chip_mate(step) * 2 + (1 - my_core)],
            pair_recv.at[step],
            e_ss.at[step],
            e_rs.at[step],
            pb=partner,
        )
        copy.start()
        pair_copies.append(copy)

    if n_chip <= 2:
        for step in range(0, n_pb):
            score(pb_mate(step))
        for copy in turn_copies:
            copy.wait_recv()
        total = interact(my_pb, total)
        for step in range(1, n_chip):
            for core in range(2):
                total = interact(chip_mate(step) * 2 + core, total)
            send_pair(step)
        total = interact(partner, total)
        send_pair(0)
    else:
        for copy in turn_copies:
            copy.wait_recv()
        lax.fori_loop(0, n_pb, lambda p, c: (score(p), c)[1], 0)
        total = lax.fori_loop(0, n_pb, interact, total)
        for step in list(range(1, n_chip)) + [0]:
            send_pair(step)
    q_part[...] = total.reshape(q_part.shape)
    q_code[...], q_peak[...] = encode(total.reshape(q_part.shape))

    out_copies, peak_copies = [], []
    for step in far_first:
        mate = dev_mate(step)
        copy = remote(
            q_peak.at[mate], q_recv_peak.at[my_dev], rp_ss.at[step], rp_rs.at[step], dev=mate
        )
        copy.start()
        peak_copies.append(copy)
        copy = remote(q_code.at[mate], q_recv.at[my_dev], r_ss.at[step], r_rs.at[step], dev=mate)
        copy.start()
        out_copies.append(copy)

    chip_copies, chip_peak_copies = [], []
    for step in range(1, n_chip):
        pair_copies[step - 1].wait_recv()
        mate = chip_mate(step) * 2 + my_core
        pair_sum = doc_part[mate] + pair_recv[step]
        pair_code[step], pair_peak[step] = encode(
            pair_sum.reshape(own_docs, slots, pair_sum.shape[1])
        )
        copy = remote(
            pair_peak.at[step], chip_peak.at[step], cp_ss.at[step], cp_rs.at[step], pb=mate
        )
        copy.start()
        chip_peak_copies.append(copy)
        copy = remote(
            pair_code.at[step], chip_code.at[step], c_ss.at[step], c_rs.at[step], pb=mate
        )
        copy.start()
        chip_copies.append(copy)
    pair_copies[-1].wait_recv()
    doc_total = doc_part[my_pb] + pair_recv[0]
    doc_total = doc_total.reshape(own_docs, slots, doc_total.shape[1])
    for step in range(1, n_chip):
        chip_copies[step - 1].wait_recv()
        chip_peak_copies[step - 1].wait_recv()
        doc_total = doc_total + decode(chip_code[step], chip_peak[step])
    for k in range(own_docs):
        span = slice(k * slots, (k + 1) * slots)
        doc_out[span, :] = jnp.where(slot < lengths[k], doc_total[k], 0.0)

    query_total = q_part[my_dev]
    for step, copy, peak_copy in reversed(list(zip(far_first, out_copies, peak_copies))):
        copy.wait_recv()
        peak_copy.wait_recv()
        mate = dev_mate(step)
        query_total = query_total + decode(q_recv[mate], q_recv_peak[mate])
    query_out[...] = query_total

    for copy in (
        aux_copies + q_copies + d_copies + turn_copies + pair_copies + out_copies + chip_copies
        + peak_copies + chip_peak_copies
    ):
        copy.wait_send()


def per_device(queries, documents, lengths, normalizers, probs, positives):
    n_pb, n_dev = lax.axis_size("pb"), lax.axis_size("dev")
    tokens, width = queries.shape
    rows = documents.shape[0]
    own_docs = lengths.shape[0]
    block = normalizers.shape[1]
    n_chip = n_pb // 2
    bf16 = jnp.bfloat16
    dma = pltpu.SemaphoreType.DMA
    hbm = pl.BlockSpec(memory_space=pl.ANY)
    vmem = pl.BlockSpec(memory_space=pltpu.VMEM)
    return pl.pallas_call(
        functools.partial(kernel, n_pb, n_dev),
        out_shape=(
            pltpu.VMEM((tokens, width), F32),
            pltpu.VMEM((rows, width), F32),
        ),
        in_specs=[hbm] * 6,
        out_specs=(vmem, vmem),
        scratch_shapes=[
            pltpu.SMEM(lengths.shape, jnp.int32),
            pltpu.VMEM(probs.shape, F32),
            pltpu.SMEM(positives.shape, jnp.int32),
            pltpu.VMEM((n_pb, rows, n_dev * tokens), F32),
            pltpu.VMEM((tokens, width), bf16),
            pltpu.VMEM((rows, width), bf16),
            pltpu.VMEM(normalizers.shape, F32),
            pltpu.VMEM((n_dev, tokens, width), bf16),
            pltpu.VMEM((n_pb, rows, width), bf16),
            pltpu.VMEM((n_dev, 2 * own_docs, block), F32),
            pltpu.VMEM((n_dev, 2 * own_docs, block), F32),
            pltpu.VMEM((n_pb, 2 * own_docs, n_dev * tokens), F32),
            pltpu.VMEM((n_pb, 2 * own_docs, n_dev * tokens), F32),
            pltpu.VMEM((n_pb, rows, width), F32),
            pltpu.VMEM((n_chip, rows, width), F32),
            pltpu.VMEM((n_chip, own_docs, rows // own_docs, width), jnp.int16),
            pltpu.VMEM((n_chip, own_docs, 1, width), F32),
            pltpu.VMEM((n_chip, own_docs, rows // own_docs, width), jnp.int16),
            pltpu.VMEM((n_chip, own_docs, 1, width), F32),
            pltpu.VMEM((n_dev, tokens, width), F32),
            pltpu.VMEM((n_dev, tokens, width), jnp.int16),
            pltpu.VMEM((n_dev, 1, width), F32),
            pltpu.VMEM((n_dev, tokens, width), jnp.int16),
            pltpu.VMEM((n_dev, 1, width), F32),
            dma((6,)),
        ]
        + [dma((n_dev,))] * 4
        + [dma((n_pb,))] * 4
        + [dma((n_chip,))] * 4
        + [dma((n_dev,))] * 4
        + [dma((n_chip,))] * 2,
        compiler_params=pltpu.CompilerParams(collective_id=0, has_side_effects=True),
    )(queries, documents, lengths, normalizers, probs, positives)


def solution(mesh):
    in_specs = (
        P(("dev", "pb"), None),
        P(("pb", "dev"), None),
        P(("pb", "dev")),
        P("pb", "dev"),
        P("dev", "pb"),
        P("dev"),
    )
    out_specs = (P(("dev", "pb"), None), P(("pb", "dev"), None))
    return jax.shard_map(
        per_device, mesh=mesh, in_specs=in_specs, out_specs=out_specs, check_vma=False
    )
```

```python
import functools

import jax
import jax.numpy as jnp
from jax import lax
from jax.experimental import pallas as pl
from jax.experimental.pallas import tpu as pltpu
from jax.sharding import PartitionSpec as P

sharpness = 10.0
MESH = pl.DeviceIdType.MESH
F32 = jnp.float32


LEVELS = 32000.0


def encode(part):
    peak = jnp.maximum(jnp.max(jnp.abs(part), axis=1, keepdims=True), 1e-30)
    return jnp.round(part * (LEVELS / peak)).astype(jnp.int32).astype(jnp.int16), peak


def decode(code, peak):
    return code.astype(jnp.int32).astype(F32) * (peak * (1.0 / LEVELS))


def kernel(
    n_pb,
    n_dev,
    queries,
    documents,
    lengths_in,
    normalizers,
    probs_in,
    positives_in,
    query_out,
    doc_out,
    lengths,
    probs,
    positives,
    scores,
    q_own,
    d_own,
    z_own,
    q_all,
    d_all,
    aux_send,
    aux_recv,
    aux_turn,
    aux_all,
    doc_part,
    pair_recv,
    pair_code,
    pair_peak,
    chip_code,
    chip_peak,
    q_part,
    q_code,
    q_peak,
    q_recv,
    q_recv_peak,
    in_sem,
    q_ss,
    q_rs,
    a_ss,
    a_rs,
    d_ss,
    d_rs,
    t_ss,
    t_rs,
    e_ss,
    e_rs,
    c_ss,
    c_rs,
    r_ss,
    r_rs,
    rp_ss,
    rp_rs,
    cp_ss,
    cp_rs,
):
    my_pb = lax.axis_index("pb")
    my_dev = lax.axis_index("dev")
    own_docs = lengths.shape[0]
    slots = d_own.shape[0] // own_docs
    row_docs, block = z_own.shape
    tokens = q_own.shape[0]
    block_queries = probs.shape[0]
    query_length = block // block_queries
    n_chip = n_pb // 2
    my_chip, my_core = my_pb // 2, my_pb % 2
    partner = my_chip * 2 + (1 - my_core)

    def crossed(place, step, count):
        mate, bit = 0, 1
        while bit < count:
            mate = mate + bit * ((place // bit + step // bit) % 2)
            bit *= 2
        return mate

    def dev_mate(step):
        return crossed(my_dev, step, n_dev)

    def pb_mate(step):
        return crossed(my_pb, step, n_pb)

    def chip_mate(step):
        return crossed(my_chip, step, n_chip)

    def remote(src, dst, send, recv, pb=None, dev=None):
        return pltpu.make_async_remote_copy(
            src_ref=src,
            dst_ref=dst,
            send_sem=send,
            recv_sem=recv,
            device_id=(my_pb if pb is None else pb, my_dev if dev is None else dev),
            device_id_type=MESH,
        )

    barrier = pltpu.get_barrier_semaphore()
    far_first = list(range(n_dev - 1, 0, -1))
    for step in far_first:
        pl.semaphore_signal(
            barrier, inc=1, device_id=(my_pb, dev_mate(step)), device_id_type=MESH
        )
    for step in range(1, n_pb):
        pl.semaphore_signal(
            barrier, inc=1, device_id=(pb_mate(step), my_dev), device_id_type=MESH
        )

    loads = [
        pltpu.make_async_copy(queries, q_own, in_sem.at[0]),
        pltpu.make_async_copy(documents, d_own, in_sem.at[1]),
        pltpu.make_async_copy(normalizers, z_own, in_sem.at[2]),
        pltpu.make_async_copy(lengths_in, lengths, in_sem.at[3]),
        pltpu.make_async_copy(probs_in, probs, in_sem.at[4]),
        pltpu.make_async_copy(positives_in, positives, in_sem.at[5]),
    ]
    for load in loads:
        load.start()
    for load in loads:
        load.wait()

    place0 = lax.broadcasted_iota(jnp.int32, (row_docs, row_docs), 0)
    place1 = lax.broadcasted_iota(jnp.int32, (row_docs, row_docs), 1)
    doc_ids = my_pb * row_docs + lax.broadcasted_iota(jnp.int32, (row_docs, 1), 0)
    query_of = lax.broadcasted_iota(jnp.int32, (1, block), 1) // query_length
    signal = jnp.zeros((row_docs, block), F32)
    for k in range(block_queries):
        column = jnp.sum(
            jnp.where(place0 == place1, probs[k : k + 1, :], 0.0), axis=1, keepdims=True
        )
        column = column - (doc_ids == positives[k]).astype(F32)
        signal = jnp.where(query_of == k, column, signal)
    for e in range(n_dev):
        span = slice(e * own_docs, (e + 1) * own_docs)
        aux_send[e, 0:own_docs, :] = z_own[span, :]
        aux_send[e, own_docs : 2 * own_docs, :] = signal[span, :]
    aux_recv[0] = aux_send[my_dev]
    q_all[0] = q_own[...]

    slot = lax.broadcasted_iota(jnp.int32, (slots, 1), 0)
    for k in range(own_docs):
        span = slice(k * slots, (k + 1) * slots)
        rows = d_own[span, :].astype(F32)
        d_all[my_pb, span, :] = jnp.where(slot < lengths[k], rows, 0.0).astype(jnp.bfloat16)

    pl.semaphore_wait(barrier, n_dev - 1 + n_pb - 1)

    aux_copies, q_copies, d_copies = [], [], []
    for step in far_first:
        mate = dev_mate(step)
        copy = remote(
            aux_send.at[mate], aux_recv.at[step], a_ss.at[step], a_rs.at[step], dev=mate
        )
        copy.start()
        aux_copies.append(copy)
    for step in far_first:
        copy = remote(q_own, q_all.at[step], q_ss.at[step], q_rs.at[step], dev=dev_mate(step))
        copy.start()
        q_copies.append(copy)
    for step in range(1, n_pb):
        copy = remote(
            d_all.at[my_pb], d_all.at[my_pb], d_ss.at[step], d_rs.at[step], pb=pb_mate(step)
        )
        copy.start()
        d_copies.append(copy)

    for copy in aux_copies:
        copy.wait_recv()
    for p in range(n_pb):
        for e in range(n_dev):
            aux_turn[p, :, e * tokens : (e + 1) * tokens] = aux_recv[
                e, :, p * tokens : (p + 1) * tokens
            ]
    aux_all[my_pb] = aux_turn[my_pb]
    turn_copies = []
    for step in range(1, n_pb):
        mate = pb_mate(step)
        copy = remote(
            aux_turn.at[mate], aux_all.at[my_pb], t_ss.at[step], t_rs.at[step], pb=mate
        )
        copy.start()
        turn_copies.append(copy)

    for copy in q_copies + d_copies:
        copy.wait_recv()

    q_rows = q_all[...].reshape(n_dev * tokens, q_own.shape[1])

    def score(p):
        scores[p] = lax.dot_general(
            d_all[p], q_rows, (((1,), (1,)), ((), ())), preferred_element_type=F32
        )

    half = n_dev // 2 * tokens

    def interact(p, total, far):
        span = slice(half, 2 * half) if far else slice(0, half)
        d_rows = d_all[p]
        aux = aux_all[p]
        parts = []
        for k in range(own_docs):
            shifted = sharpness * scores[p, k * slots : (k + 1) * slots, span] - aux[k : k + 1, span]
            weight = jnp.exp(jnp.minimum(shifted, 0.0)) * aux[own_docs + k : own_docs + k + 1, span]
            parts.append(weight.astype(jnp.bfloat16))
        weight = jnp.concatenate(parts, axis=0)
        part = jnp.dot(weight, q_rows[span, :], preferred_element_type=F32)
        doc_part[p] = part if far else doc_part[p] + part
        return total + lax.dot_general(
            weight, d_rows, (((0,), (0,)), ((), ())), preferred_element_type=F32
        )

    zero = jnp.zeros((half, q_own.shape[1]), F32)
    pair_copies = []

    def send_pair(step):
        copy = remote(
            doc_part.at[chip_mate(step) * 2 + (1 - my_core)],
            pair_recv.at[step],
            e_ss.at[step],
            e_rs.at[step],
            pb=partner,
        )
        copy.start()
        pair_copies.append(copy)

    out_copies, peak_copies = [], []

    def send_half(total, far):
        first = n_dev // 2 if far else 0
        rows = total.reshape(n_dev // 2, tokens, total.shape[1])
        span = slice(first, first + n_dev // 2)
        if not far:
            q_part[...] = rows[0]
        q_code[span], q_peak[span] = encode(rows)
        for step in range(first + n_dev // 2 - 1, max(first, 1) - 1, -1):
            mate = dev_mate(step)
            copy = remote(
                q_peak.at[step], q_recv_peak.at[step], rp_ss.at[step], rp_rs.at[step], dev=mate
            )
            copy.start()
            peak_copies.append(copy)
            copy = remote(q_code.at[step], q_recv.at[step], r_ss.at[step], r_rs.at[step], dev=mate)
            copy.start()
            out_copies.append(copy)

    if n_chip <= 2:
        for step in range(0, n_pb):
            score(pb_mate(step))
        for copy in turn_copies:
            copy.wait_recv()
        total = zero
        for step in range(n_pb - 1, -1, -1):
            total = interact(pb_mate(step), total, True)
        send_half(total, True)
        total = zero
        for step in range(1, n_chip):
            for core in range(2):
                total = interact(chip_mate(step) * 2 + core, total, False)
            send_pair(step)
        total = interact(partner, total, False)
        send_pair(0)
        total = interact(my_pb, total, False)
    else:
        for copy in turn_copies:
            copy.wait_recv()
        lax.fori_loop(0, n_pb, lambda p, c: (score(p), c)[1], 0)
        total = lax.fori_loop(0, n_pb, lambda p, c: interact(p, c, True), zero)
        send_half(total, True)
        total = lax.fori_loop(0, n_pb, lambda p, c: interact(p, c, False), zero)
        for step in list(range(1, n_chip)) + [0]:
            send_pair(step)
    send_half(total, False)

    chip_copies, chip_peak_copies = [], []
    for step in range(1, n_chip):
        pair_copies[step - 1].wait_recv()
        mate = chip_mate(step) * 2 + my_core
        pair_sum = doc_part[mate] + pair_recv[step]
        pair_code[step], pair_peak[step] = encode(
            pair_sum.reshape(own_docs, slots, pair_sum.shape[1])
        )
        copy = remote(
            pair_peak.at[step], chip_peak.at[step], cp_ss.at[step], cp_rs.at[step], pb=mate
        )
        copy.start()
        chip_peak_copies.append(copy)
        copy = remote(
            pair_code.at[step], chip_code.at[step], c_ss.at[step], c_rs.at[step], pb=mate
        )
        copy.start()
        chip_copies.append(copy)
    pair_copies[-1].wait_recv()
    doc_total = doc_part[my_pb] + pair_recv[0]
    doc_total = doc_total.reshape(own_docs, slots, doc_total.shape[1])
    for step in range(1, n_chip):
        chip_copies[step - 1].wait_recv()
        chip_peak_copies[step - 1].wait_recv()
        doc_total = doc_total + decode(chip_code[step], chip_peak[step])
    for k in range(own_docs):
        span = slice(k * slots, (k + 1) * slots)
        doc_out[span, :] = jnp.where(slot < lengths[k], doc_total[k], 0.0)

    query_total = q_part[...]
    for step, copy, peak_copy in reversed(list(zip(far_first, out_copies, peak_copies))):
        copy.wait_recv()
        peak_copy.wait_recv()
        query_total = query_total + decode(q_recv[step], q_recv_peak[step])
    query_out[...] = query_total

    for copy in (
        aux_copies + q_copies + d_copies + turn_copies + pair_copies + out_copies + chip_copies
        + peak_copies + chip_peak_copies
    ):
        copy.wait_send()


def per_device(queries, documents, lengths, normalizers, probs, positives):
    n_pb, n_dev = lax.axis_size("pb"), lax.axis_size("dev")
    tokens, width = queries.shape
    rows = documents.shape[0]
    own_docs = lengths.shape[0]
    block = normalizers.shape[1]
    n_chip = n_pb // 2
    bf16 = jnp.bfloat16
    dma = pltpu.SemaphoreType.DMA
    hbm = pl.BlockSpec(memory_space=pl.ANY)
    vmem = pl.BlockSpec(memory_space=pltpu.VMEM)
    return pl.pallas_call(
        functools.partial(kernel, n_pb, n_dev),
        out_shape=(
            pltpu.VMEM((tokens, width), F32),
            pltpu.VMEM((rows, width), F32),
        ),
        in_specs=[hbm] * 6,
        out_specs=(vmem, vmem),
        scratch_shapes=[
            pltpu.SMEM(lengths.shape, jnp.int32),
            pltpu.VMEM(probs.shape, F32),
            pltpu.SMEM(positives.shape, jnp.int32),
            pltpu.VMEM((n_pb, rows, n_dev * tokens), F32),
            pltpu.VMEM((tokens, width), bf16),
            pltpu.VMEM((rows, width), bf16),
            pltpu.VMEM(normalizers.shape, F32),
            pltpu.VMEM((n_dev, tokens, width), bf16),
            pltpu.VMEM((n_pb, rows, width), bf16),
            pltpu.VMEM((n_dev, 2 * own_docs, block), F32),
            pltpu.VMEM((n_dev, 2 * own_docs, block), F32),
            pltpu.VMEM((n_pb, 2 * own_docs, n_dev * tokens), F32),
            pltpu.VMEM((n_pb, 2 * own_docs, n_dev * tokens), F32),
            pltpu.VMEM((n_pb, rows, width), F32),
            pltpu.VMEM((n_chip, rows, width), F32),
            pltpu.VMEM((n_chip, own_docs, rows // own_docs, width), jnp.int16),
            pltpu.VMEM((n_chip, own_docs, 1, width), F32),
            pltpu.VMEM((n_chip, own_docs, rows // own_docs, width), jnp.int16),
            pltpu.VMEM((n_chip, own_docs, 1, width), F32),
            pltpu.VMEM((tokens, width), F32),
            pltpu.VMEM((n_dev, tokens, width), jnp.int16),
            pltpu.VMEM((n_dev, 1, width), F32),
            pltpu.VMEM((n_dev, tokens, width), jnp.int16),
            pltpu.VMEM((n_dev, 1, width), F32),
            dma((6,)),
        ]
        + [dma((n_dev,))] * 4
        + [dma((n_pb,))] * 4
        + [dma((n_chip,))] * 4
        + [dma((n_dev,))] * 4
        + [dma((n_chip,))] * 2,
        compiler_params=pltpu.CompilerParams(collective_id=0, has_side_effects=True),
    )(queries, documents, lengths, normalizers, probs, positives)


def solution(mesh):
    in_specs = (
        P(("dev", "pb"), None),
        P(("pb", "dev"), None),
        P(("pb", "dev")),
        P("pb", "dev"),
        P("dev", "pb"),
        P("dev"),
    )
    out_specs = (P(("dev", "pb"), None), P(("pb", "dev"), None))
    return jax.shard_map(
        per_device, mesh=mesh, in_specs=in_specs, out_specs=out_specs, check_vma=False
    )
```
